128 devices in a mesh: rep: 4 (over x), tile: 32 (over z, y, core).
Axes of the slice: x: 4, y: 4, z: 4, core: 2. Of those that a mesh axis runs over, the one named last changes fastest.
Arguments:
- feature_tiles: bfloat16 [256, 16, 128, 128], P(('rep', 'tile')), parts along dimension 0, may hold values from -6 to 6
- neighbours: int32 [256, 4], P('rep'), parts along dimension 0, may hold values from -1 to 63, as said below
- valid_rows: int32 [256], P('rep'), parts along dimension 0, may hold values from 4 to 16, as said below
- tile_image: int32 [256], P('rep'), parts along dimension 0, may hold values from 0 to 31, as said below
- gain_one: float32 [128], replicated, may hold values from 0.1 to 1.9
- shift_one: float32 [128], replicated, may hold values from -3 to 3
- kernel_one: bfloat16 [3, 3, 128, 128], replicated, may hold values from -0.1875 to 0.1875
- offset_one: float32 [128], replicated, may hold values from -3 to 3
- gain_two: float32 [128], replicated, may hold values from 0.1 to 1.9
- shift_two: float32 [128], replicated, may hold values from -3 to 3
- kernel_two: bfloat16 [3, 3, 128, 128], replicated, may hold values from -0.1875 to 0.1875
- offset_two: float32 [128], replicated, may hold values from -3 to 3
Outputs:
- block_out: bfloat16 [256, 16, 128, 128], P(('rep', 'tile')), parts along dimension 0
The draws below stay inside these ranges and needn't reach their ends.
There are 4 independent parts, one for each index of `rep`. The reference program is written for one: setup_inputs(seed, part) draws one part's arguments, and reference() takes and returns one part's arrays. A program takes and returns all parts, laid end to end along the dimension named above; an argument that names none is the same for every part. Nothing has to cross between parts.
Inputs may be any that keep to these rules, and one draw needn't show every extreme that they name: Each image is a rectangle of tiles; neighbours name the adjacent tile of the same image in that direction, or -1 at the image's border. `valid_rows`: only tiles in the bottom row of tiles of an image have fewer than 16 rows; all tiles of that row have the same count. `tile_image`: image numbers need not be consecutive; some may be unused.
All inputs are finite; a program needn't handle non-finite values.
Results may differ from the reference program's by a relative error of at most 0.0075.
Values may be sent and summed in bfloat16 or wider, within the bound.
A program may use at most 64 MiB of HBM per device.

```python
import jax
import jax.numpy as jnp
from jax import lax

C = 128
G = 32
TH = 16
TW = 128
NT = 64
IMAGES = 32


def layout(key):
    folded = jax.random.fold_in(key, 7)
    key_start, key_cut, key_rows, key_order = jax.random.split(folded, 4)
    band_rows = NT // 4
    starts = jax.random.randint(key_start, (band_rows,), 0, 2).astype(jnp.int32).at[0].set(1)
    band_of = jnp.cumsum(starts) - 1
    cut_col = jax.random.randint(key_cut, (band_rows,), 1, 5).astype(jnp.int32)[band_of]
    column = jnp.arange(4, dtype=jnp.int32)
    image_of = band_of[:, None] * 2 + (column[None, :] >= cut_col[:, None]).astype(jnp.int32)
    top_image = jnp.max(image_of)
    image_of = jnp.where(image_of == top_image, NT // 2 - 1, image_of).astype(jnp.int32)
    ending = jnp.concatenate([starts[1:], jnp.ones((1,), jnp.int32)])
    drawn_rows = jax.random.randint(key_rows, (band_rows,), TH // 4, TH + 1).astype(jnp.int32)[band_of]
    row_count = jnp.where(ending == 1, drawn_rows, TH)
    row_grid = jnp.broadcast_to(row_count[:, None], (band_rows, 4))
    canonical = jnp.arange(band_rows, dtype=jnp.int32)[:, None] * 4 + column[None, :]
    upper_slot = jnp.where(starts[:, None] == 0, canonical - 4, -1)
    lower_slot = jnp.where(ending[:, None] == 0, canonical + 4, -1)
    left_image = jnp.concatenate([jnp.full((band_rows, 1), -1, jnp.int32), image_of[:, :-1]], axis=1)
    right_image = jnp.concatenate([image_of[:, 1:], jnp.full((band_rows, 1), -1, jnp.int32)], axis=1)
    left_slot = jnp.where(left_image == image_of, canonical - 1, -1)
    right_slot = jnp.where(right_image == image_of, canonical + 1, -1)
    order_map = jax.random.permutation(key_order, NT).astype(jnp.int32)
    linked = jnp.stack([upper_slot, lower_slot, left_slot, right_slot], axis=-1).reshape(NT, 4)
    linked = jnp.where(linked >= 0, order_map[jnp.maximum(linked, 0)], -1)
    neighbour_table = jnp.zeros((NT, 4), jnp.int32).at[order_map].set(linked)
    rows_table = jnp.zeros((NT,), jnp.int32).at[order_map].set(row_grid.reshape(NT))
    image_table = jnp.zeros((NT,), jnp.int32).at[order_map].set(image_of.reshape(NT))
    return (neighbour_table, rows_table, image_table)


def draw_neighbours(key, part):
    return layout(key)[0]


def draw_valid_rows(key, part):
    return layout(key)[1]


def draw_tile_image(key, part):
    return layout(key)[2]


def steps_of(rng, extent, shards, smallest, top_value):
    gain, own = 1.0, jax.random.fold_in(rng, 6)
    for position, parts in shards:
        heights = jnp.exp(jax.random.uniform(jax.random.fold_in(own, position), (parts,), jnp.float32, smallest / len(shards), top_value / len(shards)))
        gain = gain * jnp.repeat(heights, extent[position] // parts).reshape([-1 if axis == position else 1 for axis in range(len(extent))])
    return gain


def normal_values(stream_key, shape, spread, limit, pieces=(), kind=jnp.bfloat16):
    values = jax.random.normal(stream_key, shape, jnp.float32) * spread
    if len(pieces) > 0:
        values = steps_of(stream_key, shape, pieces, -0.22, 0.18) * values
    return jnp.clip(values, min=-limit, max=limit).astype(kind)


def setup_inputs(seed: int = 0, part: int = 0) -> dict:
    splits = jax.random.split(jax.random.key(seed), 13)
    part_keys = jax.random.split(jax.random.fold_in(splits[12], part), 13)
    return {
        "feature_tiles": normal_values(part_keys[0], (NT, TH, TW, C), 1.0, 6.0, ((0, 32),)),
        "neighbours": draw_neighbours(jax.random.fold_in(jax.random.fold_in(splits[12], part), 71), part),
        "valid_rows": draw_valid_rows(jax.random.fold_in(jax.random.fold_in(splits[12], part), 71), part),
        "tile_image": draw_tile_image(jax.random.fold_in(jax.random.fold_in(splits[12], part), 71), part),
        "gain_one": jnp.clip(1.0 + 0.18 * jax.random.normal(splits[4], (C,), jnp.float32), 0.1, 1.9),
        "shift_one": normal_values(splits[5], (C,), 0.5, 3.0, (), jnp.float32),
        "kernel_one": normal_values(splits[6], (3, 3, C, C), (9 * C) ** -0.5, 0.1875),
        "offset_one": normal_values(splits[7], (C,), 0.5, 3.0, (), jnp.float32),
        "gain_two": jnp.clip(1.0 + 0.18 * jax.random.normal(splits[8], (C,), jnp.float32), 0.1, 1.9),
        "shift_two": normal_values(splits[9], (C,), 0.5, 3.0, (), jnp.float32),
        "kernel_two": normal_values(splits[10], (3, 3, C, C), (9 * C) ** -0.5, 0.1875),
        "offset_two": normal_values(splits[11], (C,), 0.5, 3.0, (), jnp.float32),
    }


epsilon = 1e-06

def pick(source, indices):
    clamped = jnp.maximum(indices, 0).astype(jnp.int32)
    fetched = jnp.take(source, clamped, axis=0)
    present = (indices >= 0).reshape(indices.shape + (1,) * (fetched.ndim - 1))
    return jnp.where(present, fetched, jnp.zeros_like(fetched))

def widen(feature, neighbours):
    left_col = pick(feature[:, :, -1, :], neighbours[:, 2])
    right_col = pick(feature[:, :, 0, :], neighbours[:, 3])
    widened = jnp.concatenate([left_col[:, :, None], feature, right_col[:, :, None]], axis=2)
    upper_row = pick(widened[:, -1], neighbours[:, 0])
    lower_row = pick(widened[:, 0], neighbours[:, 1])
    return jnp.concatenate([upper_row[:, None], widened, lower_row[:, None]], axis=1)

def convolve(padded, kernel, offset):
    tile_count, rows_pad, cols_pad, channels = padded.shape
    tile_rows, tile_cols = (rows_pad - 2, cols_pad - 2)
    summed = jnp.zeros((tile_count * tile_rows * tile_cols, kernel.shape[3]), jnp.float32)
    for row_off in range(3):
        for col_off in range(3):
            window = padded[:, row_off:row_off + tile_rows, col_off:col_off + tile_cols, :].reshape(-1, channels)
            summed = summed + jnp.dot(window, kernel[row_off, col_off], preferred_element_type=jnp.float32)
    return summed.reshape(tile_count, tile_rows, tile_cols, -1) + offset

def group_sums(per_tile, member, groups):
    images = jnp.dot(member.T, per_tile, precision=lax.Precision.HIGHEST)
    return images.reshape(images.shape[0], groups, -1).sum(axis=2)

def to_tiles(per_group, member, group_width):
    per_channel = jnp.repeat(per_group, group_width, axis=1)
    return jnp.dot(member, per_channel, precision=lax.Precision.HIGHEST)

def normalize(feature, row_mask, member, counts, gain_vec, shift_vec):
    group_width = feature.shape[3] // G
    mask_full = row_mask[:, :, None, None]
    masked = feature * mask_full
    means = group_sums(lax.optimization_barrier(jnp.sum(masked, axis=(1, 2))), member, G) / counts
    centred = (feature - to_tiles(means, member, group_width)[:, None, None, :]) * mask_full
    variance = group_sums(lax.optimization_barrier(jnp.sum(centred * centred, axis=(1, 2))), member, G) / counts
    inverse = lax.rsqrt(to_tiles(variance, member, group_width) + epsilon)
    normed = centred * inverse[:, None, None, :] * gain_vec + shift_vec
    return (jax.nn.silu(normed) * mask_full).astype(jnp.bfloat16)

def reference(feature_tiles, neighbours, valid_rows, tile_image, gain_one, shift_one, kernel_one, offset_one, gain_two, shift_two, kernel_two, offset_two):
    row_mask = (jnp.arange(TH)[None, :] < valid_rows[:, None]).astype(jnp.float32)
    mask_full = row_mask[:, :, None, None]
    member = (tile_image[:, None] == jnp.arange(IMAGES)[None, :]).astype(jnp.float32)
    pixels = (valid_rows * TW).astype(jnp.float32)
    counts = jnp.maximum(jnp.dot(member.T, pixels[:, None], precision=lax.Precision.HIGHEST) * (C // G), 1.0)
    inputs = feature_tiles.astype(jnp.float32) * mask_full
    first_act = normalize(inputs, row_mask, member, counts, gain_one, shift_one)
    hidden = (convolve(widen(first_act, neighbours), kernel_one, offset_one) * mask_full).astype(jnp.bfloat16)
    second_act = normalize(hidden.astype(jnp.float32), row_mask, member, counts, gain_two, shift_two)
    mixed_out = convolve(widen(second_act, neighbours), kernel_two, offset_two)
    return ((inputs + mixed_out) * mask_full).astype(jnp.bfloat16)
```

```python
import functools

import jax
import jax.numpy as jnp
from jax import lax
from jax.experimental import pallas as pl
from jax.experimental.pallas import tpu as pltpu
from jax.sharding import PartitionSpec as P


N = 32
TILES = 64
TH = 16
TW = 128
C = 128
RING = 144
GROUP = 4
EPS = 1e-06
f32 = jnp.float32
bf16 = jnp.bfloat16


def group_total(v):
    lane = lax.broadcasted_iota(jnp.int32, v.shape, 1)
    t = v + jnp.where(lane % 2 == 0, pltpu.roll(v, C - 1, 1), pltpu.roll(v, 1, 1))
    return t + jnp.where(lane % 4 < 2, pltpu.roll(t, C - 2, 1), pltpu.roll(t, 2, 1))


def kernel(
    x_hbm, nb, vr, ti, gain1, shift1, k1, off1, gain2, shift2, k2, off2,
    out,
    xe, p1, p2, cst, c1, c2s, c2, hc, sa, sb, hid, w1, w2, ec,
    st_send, st, wgt, cnt,
    x_sem, w_sem, p1_send, p1_recv, p2_send, p2_recv, c1_send, c1_recv, c2_send, c2_recv, st_ssem, st_rsem,
):
    me = lax.axis_index("tile")

    barrier = pltpu.get_barrier_semaphore()

    def greet(o, _):
        pl.semaphore_signal(barrier, inc=1, device_id={"tile": lax.rem(me + o, N)}, device_id_type=pl.DeviceIdType.MESH)
        return 0

    lax.fori_loop(1, N, greet, 0)

    x_copy = pltpu.make_async_copy(x_hbm, xe.at[:, 2 : 2 + TH], x_sem)
    x_copy.start()
    w_copies = []
    for conv, (k_hbm, w) in enumerate(((k1, w1), (k2, w2))):
        for half in range(2):
            for e in range(2):
                for o in range(2):
                    a = 2 * half + e - o
                    if 0 <= a <= 2:
                        w_copies.append(
                            pltpu.make_async_copy(
                                k_hbm.at[a],
                                w.at[half, pl.ds(384 * e, 384), pl.ds(128 * o, 128)],
                                w_sem.at[len(w_copies)],
                            )
                        )
    for copy in w_copies:
        copy.start()
    for w in (w1, w2):
        w[0, 0:384, 128:256] = jnp.zeros((384, 128), bf16)
        w[1, 384:768, 0:128] = jnp.zeros((384, 128), bf16)
    hc[...] = jnp.zeros(hc.shape, f32)

    x_copy.wait()

    for t in range(2):
        for side in range(2):
            block = xe[t, 2 : 2 + TH, 112 * side : 112 * side + 16, :].astype(f32)
            ec[side] = block.reshape(TH * 16, C)
        for c in range(4):
            side, at = ((1, 14), (1, 15), (0, 0), (0, 1))[c]
            for h in range(2):
                cst[2 * c + h, t] = ec[side, pl.ds(at + 128 * h, 8, stride=16), :].astype(bf16)

    pl.semaphore_wait(barrier, N - 1)

    def source_row(q):
        return jnp.where(q < 2, 16 + q, q)

    def to_picker(o, _):
        d = lax.rem(me + o, N)
        pltpu.make_async_remote_copy(
            src_ref=xe.at[:, source_row(d // 8), pl.ds(pl.multiple_of(16 * lax.rem(d, 8), 16), 16), :],
            dst_ref=p1.at[pl.ds(2 * me, 2)],
            send_sem=p1_send,
            recv_sem=p1_recv,
            device_id={"tile": d},
            device_id_type=pl.DeviceIdType.MESH,
        ).start()
        return 0

    lax.fori_loop(1, N, to_picker, 0)
    for n in range(8):

        @pl.when(me != 4 * n)
        def _():
            pltpu.make_async_remote_copy(
                src_ref=cst.at[n],
                dst_ref=c1.at[pl.ds(2 * me, 2)],
                send_sem=c1_send,
                recv_sem=c1_recv,
                device_id={"tile": 4 * n},
                device_id_type=pl.DeviceIdType.MESH,
            ).start()

    my_q = me // 8
    my_k = pl.multiple_of(16 * lax.rem(me, 8), 16)
    for t in range(2):
        p1[2 * me + t] = xe[t, source_row(my_q), pl.ds(my_k, 16), :]

    @pl.when(lax.rem(me, 4) == 0)
    def _():
        for t in range(2):
            c1[2 * me + t] = cst[me // 4, t]

    rows = [vr[2 * me + t] for t in range(2)]
    image = [ti[2 * me + t] for t in range(2)]
    links = [[nb[2 * me + t, j] for j in range(4)] for t in range(2)]
    has = [[jnp.where(links[t][j] >= 0, 1.0, 0.0).astype(f32) for j in range(4)] for t in range(2)]

    def own_mask(t, r):
        return jnp.where(r < rows[t], 1.0, 0.0).astype(f32)

    def ring_mask(t, r):
        inside = own_mask(t, r)
        return jnp.where(r < 0, has[t][0], jnp.where(r >= TH, has[t][1], inside))

    lane = lax.broadcasted_iota(jnp.int32, (1, C), 1)
    low = (lane % 4) < 2
    even = (lane % 2) == 0

    def weigh(j, _):
        for t in range(2):
            wa = jnp.where(ti[2 * j] == image[t], 1.0, 0.0).astype(f32)
            wb = jnp.where(ti[2 * j + 1] == image[t], 1.0, 0.0).astype(f32)
            wgt[t, pl.ds(j, 1), :] = jnp.where(low, wa, wb)
        na = (vr[2 * j] * (TW * GROUP)).astype(f32)
        nb_ = (vr[2 * j + 1] * (TW * GROUP)).astype(f32)
        cnt[pl.ds(j, 1), :] = jnp.where(low, na, nb_)
        return 0

    lax.fori_loop(0, N, weigh, 0)

    def statistics(which, row, mask):
        def first(r, accs):
            return tuple(
                accs[t] + jnp.sum(row(t, r).reshape(16, 8, C), axis=0) * mask(t, r) for t in range(2)
            )

        zero = jnp.zeros((8, C), f32)
        sums = lax.fori_loop(0, TH, first, (zero, zero), unroll=2)
        both = jnp.concatenate([jnp.sum(s, axis=0, keepdims=True) for s in sums] + [jnp.zeros((6, C), f32)], axis=0)
        total = group_total(both)
        means = [total[t : t + 1] / (rows[t] * (TW * GROUP)).astype(f32) for t in range(2)]

        def second(r, accs):
            outs = []
            for t in range(2):
                d = row(t, r) - means[t]
                outs.append(accs[t] + jnp.sum((d * d).reshape(16, 8, C), axis=0) * mask(t, r))
            return tuple(outs)

        squares = lax.fori_loop(0, TH, second, (zero, zero), unroll=2)
        both2 = jnp.concatenate([jnp.sum(s, axis=0, keepdims=True) for s in squares] + [jnp.zeros((6, C), f32)], axis=0)
        total2 = group_total(both2)
        packed = jnp.where(
            low,
            jnp.where(even, total[0:1], total2[0:1]),
            jnp.where(even, total[1:2], total2[1:2]),
        )
        st_send[which] = packed
        st[which, me] = packed

        def tell(o, _):
            pltpu.make_async_remote_copy(
                src_ref=st_send.at[which],
                dst_ref=st.at[which, me],
                send_sem=st_ssem.at[which],
                recv_sem=st_rsem.at[which],
                device_id={"tile": lax.rem(me + o, N)},
                device_id_type=pl.DeviceIdType.MESH,
            ).start()
            return 0

        lax.fori_loop(1, N, tell, 0)

    def scales(which, gain, shift):
        got = st.at[which, pl.ds(0, N - 1)]
        pltpu.make_async_copy(got, got, st_rsem.at[which]).wait()
        all_rows = st[which].reshape(N, C)
        counts = cnt[...]
        mean_of = all_rows / counts
        result = []
        for t in range(2):
            w = wgt[t]
            s = jnp.sum(jnp.where(even, w * all_rows, 0.0), axis=0, keepdims=True)
            n = jnp.sum(jnp.where(even, w * counts, 0.0), axis=0, keepdims=True)
            sn = group_total(jnp.concatenate([s, n, jnp.zeros((6, C), f32)], axis=0))
            mean, number = sn[0:1] / sn[1:2], sn[1:2]
            d = mean_of - mean
            m2 = jnp.sum(w * jnp.where(even, counts * d * d, all_rows), axis=0, keepdims=True)
            var = group_total(jnp.concatenate([m2, jnp.zeros((7, C), f32)], axis=0))[0:1] / number
            a = lax.rsqrt(var + EPS) * gain[...]
            result.append((0.5 * a, 0.5 * (shift[...] - mean * a)))
        return result

    statistics(0, lambda t, r: xe[t, 2 + r].astype(f32), own_mask)

    got = p1.at[pl.ds(0, 2 * (N - 1))]
    pltpu.make_async_copy(got, got, p1_recv).wait()
    column = my_q // 2
    ring_row = jnp.where(my_q < 2, my_q, 16 + my_q)

    def to_owner(o, _):
        d = lax.rem(me + o, N)
        for t in range(2):
            p2[d, t] = p1[jnp.maximum(nb[2 * d + t, column], 0)]
        pltpu.make_async_remote_copy(
            src_ref=p2.at[d],
            dst_ref=xe.at[:, ring_row, pl.ds(my_k, 16), :],
            send_sem=p2_send,
            recv_sem=p2_recv,
            device_id={"tile": d},
            device_id_type=pl.DeviceIdType.MESH,
        ).start()
        return 0

    lax.fori_loop(1, N, to_owner, 0)
    for t in range(2):
        xe[t, ring_row, pl.ds(my_k, 16), :] = p1[jnp.maximum(links_of(nb, 2 * me + t, column), 0)]

    @pl.when(lax.rem(me, 4) == 0)
    def _():
        n = me // 4
        got = c1.at[pl.ds(0, 2 * (N - 1))]
        pltpu.make_async_copy(got, got, c1_recv).wait()
        side = jnp.where(n < 4, 2, 3)
        across = jnp.where(lax.rem(n, 2) == 0, 1, 0)

        def pick(d, t, j):
            if j == 0:
                return c1[jnp.maximum(nb[2 * d + t, side], 0)]
            other = jnp.maximum(nb[2 * d + t, across], 0)
            return c1[jnp.maximum(nb[other, side], 0)]

        def column_to_owner(o, _):
            d = lax.rem(me + o, N)
            for t in range(2):
                for j in range(2):
                    c2s[d, t, j] = pick(d, t, j)
            pltpu.make_async_remote_copy(
                src_ref=c2s.at[d],
                dst_ref=c2.at[n],
                send_sem=c2_send,
                recv_sem=c2_recv,
                device_id={"tile": d},
                device_id_type=pl.DeviceIdType.MESH,
            ).start()
            return 0

        lax.fori_loop(1, N, column_to_owner, 0)
        for t in range(2):
            for j in range(2):
                c2[n, t, j] = pick(me, t, j)
        got = c2.at[pl.ds(0, 7)]
        pltpu.make_async_copy(got, got, c2_recv).wait()

    @pl.when(lax.rem(me, 4) != 0)
    def _():
        pltpu.make_async_copy(c2, c2, c2_recv).wait()

    scale1 = scales(0, gain1, shift1)
    got = p1.at[pl.ds(0, 2 * (N - 1))]
    pltpu.make_async_copy(got, got, p2_recv).wait()

    for t in range(2):
        for c in range(4):
            at = (14, 15, 0, 1)[c]
            for h in range(2):
                hc[t, pl.ds(16 * (2 + 8 * h) + at, 8, stride=16), :] = c2[2 * c + h, t, 0].astype(f32)
            hc[t, pl.ds(at, 2, stride=16), :] = c2[2 * c + 1, t, 1].astype(f32)[6:8]
            hc[t, pl.ds(16 * 18 + at, 2, stride=16), :] = c2[2 * c, t, 1].astype(f32)[0:2]

    place = lax.broadcasted_iota(jnp.int32, (16, 1), 0)
    sides = [jnp.where(place < 8, has[t][3], has[t][2]) for t in range(2)]

    def activate(v, a, b):
        u = v * a + b
        return u * jnp.tanh(u) + u

    def norm1(p, _):
        for t in range(2):
            a, b = scale1[t]
            for e in range(2):
                i = 2 * p + e
                m = ring_mask(t, i - 2)
                am, bm = a * m, b * m
                mid = activate(xe[t, i].astype(f32), am, bm)
                end = activate(hc[t, pl.ds(pl.multiple_of(16 * i, 16), 16), :], am * sides[t], bm * sides[t])
                full = jnp.concatenate([mid, end], axis=0)
                before = pltpu.roll(full, 1, 0)
                after = pltpu.roll(full, RING - 1, 0)
                for s, v in enumerate((before, full, after)):
                    sa[t, p, :, pl.ds(384 * e + 128 * s, 128)] = v.astype(bf16)
        return 0

    lax.fori_loop(0, 10, norm1, 0)
    for copy in w_copies[:6]:
        copy.wait()

    bias1 = jnp.concatenate([off1[...], off1[...]], axis=1)
    bias2 = jnp.concatenate([off2[...], off2[...]], axis=1)

    def conv1(step, _):
        t, p0 = step // 3, 3 * lax.rem(step, 3)
        acc = jnp.dot(sa[t, pl.ds(p0, 3)].reshape(3 * RING, 768), w1[0], preferred_element_type=f32)
        acc += jnp.dot(sa[t, pl.ds(p0 + 1, 3)].reshape(3 * RING, 768), w1[1], preferred_element_type=f32)
        h = (acc + bias1).astype(bf16).reshape(3, RING, 256)
        for pp in range(3):
            for e in range(2):
                hid[t, 2 * (p0 + pp) + e] = h[pp, :, 128 * e : 128 * e + 128]
        return 0

    lax.fori_loop(0, 6, conv1, 0)

    statistics(1, lambda t, r: hid[t, 1 + r, 0:TW, :].astype(f32), own_mask)
    for copy in w_copies[6:]:
        copy.wait()
    scale2 = scales(1, gain2, shift2)

    def norm2(p, _):
        for t in range(2):
            a, b = scale2[t]
            for e in range(2):
                i = 2 * p + e
                m = ring_mask(t, i - 1)
                am, bm = a * m, b * m
                h = hid[t, i].astype(f32)
                mid = activate(h[0:TW], am, bm)
                end = activate(h[TW:RING], am * sides[t], bm * sides[t])
                full = jnp.concatenate([mid, end], axis=0)
                before = pltpu.roll(full, 1, 0)
                after = pltpu.roll(full, RING - 1, 0)
                for s, v in enumerate((before, full, after)):
                    sb[t, p, :, pl.ds(384 * e + 128 * s, 128)] = v[0:TW].astype(bf16)
        return 0

    lax.fori_loop(0, 9, norm2, 0)

    def conv2(step, _):
        t, p0 = step // 2, 4 * lax.rem(step, 2)
        acc = jnp.dot(sb[t, pl.ds(p0, 4)].reshape(4 * TW, 768), w2[0], preferred_element_type=f32)
        acc += jnp.dot(sb[t, pl.ds(p0 + 1, 4)].reshape(4 * TW, 768), w2[1], preferred_element_type=f32)
        y = (acc + bias2).reshape(4, TW, 256)
        for pp in range(4):
            for e in range(2):
                r = 2 * (p0 + pp) + e
                v = y[pp, :, 128 * e : 128 * e + 128] + xe[t, 2 + r].astype(f32)
                m = jnp.where(r < jnp.where(t == 0, rows[0], rows[1]), 1.0, 0.0).astype(f32)
                out[t, r] = (v * m).astype(bf16)
        return 0

    lax.fori_loop(0, 4, conv2, 0)

    got = p1.at[pl.ds(0, 2 * (N - 1))]
    pltpu.make_async_copy(got, got, p1_send).wait()
    pltpu.make_async_copy(got, got, p2_send).wait()
    for which in range(2):
        got = st.at[which, pl.ds(0, N - 1)]
        pltpu.make_async_copy(got, got, st_ssem.at[which]).wait()

    @pl.when(lax.rem(me, 4) == 0)
    def _():
        got = cst.at[pl.ds(0, 7)]
        pltpu.make_async_copy(got, got, c1_send).wait()
        got = c2s.at[pl.ds(0, N - 1)]
        pltpu.make_async_copy(got, got, c2_send).wait()

    @pl.when(lax.rem(me, 4) != 0)
    def _():
        pltpu.make_async_copy(cst, cst, c1_send).wait()


def links_of(nb, tile, column):
    return nb[tile, column]


def shards(x, nb, vr, ti, gain1, shift1, kernel1, off1, gain2, shift2, kernel2, off2):
    vmem = pl.BlockSpec(memory_space=pltpu.VMEM)
    smem = pl.BlockSpec(memory_space=pltpu.SMEM)
    anywhere = pl.BlockSpec(memory_space=pl.ANY)
    dma = pltpu.SemaphoreType.DMA
    row = lambda v: v.reshape(1, C)
    return pl.pallas_call(
        kernel,
        out_shape=jax.ShapeDtypeStruct(x.shape, x.dtype),
        in_specs=[anywhere, smem, smem, smem, vmem, vmem, anywhere, vmem, vmem, vmem, anywhere, vmem],
        out_specs=vmem,
        scratch_shapes=[
            pltpu.VMEM((2, TH + 4, TW, C), bf16),
            pltpu.VMEM((TILES, 16, C), bf16),
            pltpu.VMEM((N, 2, 16, C), bf16),
            pltpu.VMEM((8, 2, 8, C), bf16),
            pltpu.VMEM((TILES, 8, C), bf16),
            pltpu.VMEM((N, 2, 2, 8, C), bf16),
            pltpu.VMEM((8, 2, 2, 8, C), bf16),
            pltpu.VMEM((2, 20 * 16, C), f32),
            pltpu.VMEM((2, 10, RING, 768), bf16),
            pltpu.VMEM((2, 9, TW, 768), bf16),
            pltpu.VMEM((2, 18, RING, C), bf16),
            pltpu.VMEM((2, 768, 256), bf16),
            pltpu.VMEM((2, 768, 256), bf16),
            pltpu.VMEM((2, TH * 16, C), f32),
            pltpu.VMEM((2, 1, C), f32),
            pltpu.VMEM((2, N, 1, C), f32),
            pltpu.VMEM((2, N, C), f32),
            pltpu.VMEM((N, C), f32),
            dma,
            dma((12,)),
            dma,
            dma,
            dma,
            dma,
            dma,
            dma,
            dma,
            dma,
            dma((2,)),
            dma((2,)),
        ],
        compiler_params=pltpu.CompilerParams(
            collective_id=0, has_side_effects=True, vmem_limit_bytes=48 * 1024 * 1024
        ),
    )(
        x, nb, vr, ti, row(gain1), row(shift1), kernel1.reshape(3, 3 * C, C), row(off1),
        row(gain2), row(shift2), kernel2.reshape(3, 3 * C, C), row(off2),
    )


def solution(mesh):
    in_specs = (P(("rep", "tile"), None, None, None), P("rep", None), P("rep"), P("rep")) + (P(),) * 8
    out_specs = P(("rep", "tile"), None, None, None)
    return jax.shard_map(shards, mesh=mesh, in_specs=in_specs, out_specs=out_specs, check_vma=False)
```

```python
import functools

import jax
import jax.numpy as jnp
from jax import lax
from jax.experimental import pallas as pl
from jax.experimental.pallas import tpu as pltpu
from jax.sharding import PartitionSpec as P


N = 32
TILES = 64
TH = 16
TW = 128
C = 128
RING = 144
GROUP = 4
EPS = 1e-06
f32 = jnp.float32
bf16 = jnp.bfloat16


def group_total(v):
    lane = lax.broadcasted_iota(jnp.int32, v.shape, 1)
    t = v + jnp.where(lane % 2 == 0, pltpu.roll(v, C - 1, 1), pltpu.roll(v, 1, 1))
    return t + jnp.where(lane % 4 < 2, pltpu.roll(t, C - 2, 1), pltpu.roll(t, 2, 1))


def kernel(
    x_hbm, nb_hbm, vr_hbm, ti_hbm, gain1_hbm, shift1_hbm, k1, off1_hbm, gain2_hbm, shift2_hbm, k2, off2_hbm,
    out,
    nb, vr, ti, gain1, shift1, off1, gain2, shift2, off2, xe, p1, p2, cst, c1, c2s, c2, hc, sa, sb, hid, w1, w2, ec,
    st_send, st, wgt, cnt,
    x_sem, s_sem, w_sem, p1_send, p1_recv, p2_send, p2_recv, c1_send, c1_recv, c2_send, c2_recv, st_ssem, st_rsem,
):
    me = lax.axis_index("tile")

    barrier = pltpu.get_barrier_semaphore()

    def greet(o, _):
        pl.semaphore_signal(barrier, inc=1, device_id={"tile": lax.rem(me + o, N)}, device_id_type=pl.DeviceIdType.MESH)
        return 0

    lax.fori_loop(1, N, greet, 0)

    x_copy = pltpu.make_async_copy(x_hbm, xe.at[:, 2 : 2 + TH], x_sem)
    x_copy.start()
    small_copies = [
        pltpu.make_async_copy(a, b, s_sem.at[j])
        for j, (a, b) in enumerate(
            (
                (nb_hbm, nb), (vr_hbm, vr), (ti_hbm, ti), (gain1_hbm, gain1), (shift1_hbm, shift1), (off1_hbm, off1),
                (gain2_hbm, gain2), (shift2_hbm, shift2), (off2_hbm, off2),
            )
        )
    ]
    for copy in small_copies:
        copy.start()
    w_copies = []
    for conv, (k_hbm, w) in enumerate(((k1, w1), (k2, w2))):
        for half in range(2):
            for e in range(2):
                for o in range(2):
                    a = 2 * half + e - o
                    if 0 <= a <= 2:
                        w_copies.append(
                            pltpu.make_async_copy(
                                k_hbm.at[a],
                                w.at[half, pl.ds(384 * e, 384), pl.ds(128 * o, 128)],
                                w_sem.at[len(w_copies)],
                            )
                        )
    for copy in w_copies:
        copy.start()
    for w in (w1, w2):
        w[0, 0:384, 128:256] = jnp.zeros((384, 128), bf16)
        w[1, 384:768, 0:128] = jnp.zeros((384, 128), bf16)
    hc[...] = jnp.zeros(hc.shape, f32)

    x_copy.wait()
    for copy in small_copies:
        copy.wait()

    for t in range(2):
        for side in range(2):
            block = xe[t, 2 : 2 + TH, 112 * side : 112 * side + 16, :].astype(f32)
            ec[side] = block.reshape(TH * 16, C)
        for c in range(4):
            side, at = ((1, 14), (1, 15), (0, 0), (0, 1))[c]
            for h in range(2):
                cst[2 * c + h, t] = ec[side, pl.ds(at + 128 * h, 8, stride=16), :].astype(bf16)

    pl.semaphore_wait(barrier, N - 1)

    def source_row(q):
        return jnp.where(q < 2, 16 + q, q)

    def to_picker(o, _):
        d = lax.rem(me + o, N)
        pltpu.make_async_remote_copy(
            src_ref=xe.at[:, source_row(d // 8), pl.ds(pl.multiple_of(16 * lax.rem(d, 8), 16), 16), :],
            dst_ref=p1.at[pl.ds(2 * me, 2)],
            send_sem=p1_send,
            recv_sem=p1_recv,
            device_id={"tile": d},
            device_id_type=pl.DeviceIdType.MESH,
        ).start()
        return 0

    lax.fori_loop(1, N, to_picker, 0)
    for n in range(8):

        @pl.when(me != 4 * n)
        def _():
            pltpu.make_async_remote_copy(
                src_ref=cst.at[n],
                dst_ref=c1.at[pl.ds(2 * me, 2)],
                send_sem=c1_send,
                recv_sem=c1_recv,
                device_id={"tile": 4 * n},
                device_id_type=pl.DeviceIdType.MESH,
            ).start()

    my_q = me // 8
    my_k = pl.multiple_of(16 * lax.rem(me, 8), 16)
    for t in range(2):
        p1[2 * me + t] = xe[t, source_row(my_q), pl.ds(my_k, 16), :]

    @pl.when(lax.rem(me, 4) == 0)
    def _():
        for t in range(2):
            c1[2 * me + t] = cst[me // 4, t]

    rows = [vr[2 * me + t] for t in range(2)]
    image = [ti[2 * me + t] for t in range(2)]
    links = [[nb[j, 2 * me + t] for j in range(4)] for t in range(2)]
    has = [[jnp.where(links[t][j] >= 0, 1.0, 0.0).astype(f32) for j in range(4)] for t in range(2)]

    def own_mask(t, r):
        return jnp.where(r < rows[t], 1.0, 0.0).astype(f32)

    def ring_mask(t, r):
        inside = own_mask(t, r)
        return jnp.where(r < 0, has[t][0], jnp.where(r >= TH, has[t][1], inside))

    lane = lax.broadcasted_iota(jnp.int32, (1, C), 1)
    low = (lane % 4) < 2
    even = (lane % 2) == 0

    def weigh(j, _):
        for t in range(2):
            wa = jnp.where(ti[2 * j] == image[t], 1.0, 0.0).astype(f32)
            wb = jnp.where(ti[2 * j + 1] == image[t], 1.0, 0.0).astype(f32)
            wgt[t, pl.ds(j, 1), :] = jnp.where(low, wa, wb)
        na = (vr[2 * j] * (TW * GROUP)).astype(f32)
        nb_ = (vr[2 * j + 1] * (TW * GROUP)).astype(f32)
        cnt[pl.ds(j, 1), :] = jnp.where(low, na, nb_)
        return 0

    lax.fori_loop(0, N, weigh, 0)

    def statistics(which, row, mask):
        def first(r, accs):
            return tuple(
                accs[t] + jnp.sum(row(t, r).reshape(16, 8, C), axis=0) * mask(t, r) for t in range(2)
            )

        zero = jnp.zeros((8, C), f32)
        sums = lax.fori_loop(0, TH, first, (zero, zero), unroll=2)
        both = jnp.concatenate([jnp.sum(s, axis=0, keepdims=True) for s in sums] + [jnp.zeros((6, C), f32)], axis=0)
        total = group_total(both)
        means = [total[t : t + 1] / (rows[t] * (TW * GROUP)).astype(f32) for t in range(2)]

        def second(r, accs):
            outs = []
            for t in range(2):
                d = row(t, r) - means[t]
                outs.append(accs[t] + jnp.sum((d * d).reshape(16, 8, C), axis=0) * mask(t, r))
            return tuple(outs)

        squares = lax.fori_loop(0, TH, second, (zero, zero), unroll=2)
        both2 = jnp.concatenate([jnp.sum(s, axis=0, keepdims=True) for s in squares] + [jnp.zeros((6, C), f32)], axis=0)
        total2 = group_total(both2)
        packed = jnp.where(
            low,
            jnp.where(even, total[0:1], total2[0:1]),
            jnp.where(even, total[1:2], total2[1:2]),
        )
        st_send[which] = packed
        st[which, me] = packed

        def tell(o, _):
            pltpu.make_async_remote_copy(
                src_ref=st_send.at[which],
                dst_ref=st.at[which, me],
                send_sem=st_ssem.at[which],
                recv_sem=st_rsem.at[which],
                device_id={"tile": lax.rem(me + o, N)},
                device_id_type=pl.DeviceIdType.MESH,
            ).start()
            return 0

        lax.fori_loop(1, N, tell, 0)

    def scales(which, gain, shift):
        got = st.at[which, pl.ds(0, N - 1)]
        pltpu.make_async_copy(got, got, st_rsem.at[which]).wait()
        all_rows = st[which].reshape(N, C)
        counts = cnt[...]
        mean_of = all_rows / counts
        result = []
        for t in range(2):
            w = wgt[t]
            s = jnp.sum(jnp.where(even, w * all_rows, 0.0), axis=0, keepdims=True)
            n = jnp.sum(jnp.where(even, w * counts, 0.0), axis=0, keepdims=True)
            sn = group_total(jnp.concatenate([s, n, jnp.zeros((6, C), f32)], axis=0))
            mean, number = sn[0:1] / sn[1:2], sn[1:2]
            d = mean_of - mean
            m2 = jnp.sum(w * jnp.where(even, counts * d * d, all_rows), axis=0, keepdims=True)
            var = group_total(jnp.concatenate([m2, jnp.zeros((7, C), f32)], axis=0))[0:1] / number
            a = lax.rsqrt(var + EPS) * gain[...]
            result.append((0.5 * a, 0.5 * (shift[...] - mean * a)))
        return result

    statistics(0, lambda t, r: xe[t, 2 + r].astype(f32), own_mask)

    got = p1.at[pl.ds(0, 2 * (N - 1))]
    pltpu.make_async_copy(got, got, p1_recv).wait()
    column = my_q // 2
    ring_row = jnp.where(my_q < 2, my_q, 16 + my_q)

    def to_owner(o, _):
        d = lax.rem(me + o, N)
        for t in range(2):
            p2[d, t] = p1[jnp.maximum(nb[column, 2 * d + t], 0)]
        pltpu.make_async_remote_copy(
            src_ref=p2.at[d],
            dst_ref=xe.at[:, ring_row, pl.ds(my_k, 16), :],
            send_sem=p2_send,
            recv_sem=p2_recv,
            device_id={"tile": d},
            device_id_type=pl.DeviceIdType.MESH,
        ).start()
        return 0

    lax.fori_loop(1, N, to_owner, 0)
    for t in range(2):
        xe[t, ring_row, pl.ds(my_k, 16), :] = p1[jnp.maximum(nb[column, 2 * me + t], 0)]

    @pl.when(lax.rem(me, 4) == 0)
    def _():
        n = me // 4
        got = c1.at[pl.ds(0, 2 * (N - 1))]
        pltpu.make_async_copy(got, got, c1_recv).wait()
        side = jnp.where(n < 4, 2, 3)
        across = jnp.where(lax.rem(n, 2) == 0, 1, 0)

        def pick(d, t, j):
            if j == 0:
                return c1[jnp.maximum(nb[side, 2 * d + t], 0)]
            other = jnp.maximum(nb[across, 2 * d + t], 0)
            return c1[jnp.maximum(nb[side, other], 0)]

        def column_to_owner(o, _):
            d = lax.rem(me + o, N)
            for t in range(2):
                for j in range(2):
                    c2s[d, t, j] = pick(d, t, j)
            pltpu.make_async_remote_copy(
                src_ref=c2s.at[d],
                dst_ref=c2.at[n],
                send_sem=c2_send,
                recv_sem=c2_recv,
                device_id={"tile": d},
                device_id_type=pl.DeviceIdType.MESH,
            ).start()
            return 0

        lax.fori_loop(1, N, column_to_owner, 0)
        for t in range(2):
            for j in range(2):
                c2[n, t, j] = pick(me, t, j)
        got = c2.at[pl.ds(0, 7)]
        pltpu.make_async_copy(got, got, c2_recv).wait()

    @pl.when(lax.rem(me, 4) != 0)
    def _():
        pltpu.make_async_copy(c2, c2, c2_recv).wait()

    scale1 = scales(0, gain1, shift1)
    got = p1.at[pl.ds(0, 2 * (N - 1))]
    pltpu.make_async_copy(got, got, p2_recv).wait()

    for t in range(2):
        for c in range(4):
            at = (14, 15, 0, 1)[c]
            for h in range(2):
                hc[t, pl.ds(16 * (2 + 8 * h) + at, 8, stride=16), :] = c2[2 * c + h, t, 0].astype(f32)
            hc[t, pl.ds(at, 2, stride=16), :] = c2[2 * c + 1, t, 1].astype(f32)[6:8]
            hc[t, pl.ds(16 * 18 + at, 2, stride=16), :] = c2[2 * c, t, 1].astype(f32)[0:2]

    place = lax.broadcasted_iota(jnp.int32, (16, 1), 0)
    sides = [jnp.where(place < 8, has[t][3], has[t][2]) for t in range(2)]

    def activate(v, a, b):
        u = v * a + b
        return u * jnp.tanh(u) + u

    def norm1(p, _):
        for t in range(2):
            a, b = scale1[t]
            for e in range(2):
                i = 2 * p + e
                m = ring_mask(t, i - 2)
                am, bm = a * m, b * m
                mid = activate(xe[t, i].astype(f32), am, bm)
                end = activate(hc[t, pl.ds(pl.multiple_of(16 * i, 16), 16), :], am * sides[t], bm * sides[t])
                full = jnp.concatenate([mid, end], axis=0)
                before = pltpu.roll(full, 1, 0)
                after = pltpu.roll(full, RING - 1, 0)
                for s, v in enumerate((before, full, after)):
                    sa[t, p, :, pl.ds(384 * e + 128 * s, 128)] = v.astype(bf16)
        return 0

    lax.fori_loop(0, 10, norm1, 0)
    for copy in w_copies[:6]:
        copy.wait()

    bias1 = jnp.concatenate([off1[...], off1[...]], axis=1)
    bias2 = jnp.concatenate([off2[...], off2[...]], axis=1)

    def conv1(step, _):
        t, p0 = step // 3, 3 * lax.rem(step, 3)
        acc = jnp.dot(sa[t, pl.ds(p0, 3)].reshape(3 * RING, 768), w1[0], preferred_element_type=f32)
        acc += jnp.dot(sa[t, pl.ds(p0 + 1, 3)].reshape(3 * RING, 768), w1[1], preferred_element_type=f32)
        h = (acc + bias1).astype(bf16).reshape(3, RING, 256)
        for pp in range(3):
            for e in range(2):
                hid[t, 2 * (p0 + pp) + e] = h[pp, :, 128 * e : 128 * e + 128]
        return 0

    lax.fori_loop(0, 6, conv1, 0)

    statistics(1, lambda t, r: hid[t, 1 + r, 0:TW, :].astype(f32), own_mask)
    for copy in w_copies[6:]:
        copy.wait()
    scale2 = scales(1, gain2, shift2)

    def norm2(p, _):
        for t in range(2):
            a, b = scale2[t]
            for e in range(2):
                i = 2 * p + e
                m = ring_mask(t, i - 1)
                am, bm = a * m, b * m
                h = hid[t, i].astype(f32)
                mid = activate(h[0:TW], am, bm)
                end = activate(h[TW:RING], am * sides[t], bm * sides[t])
                full = jnp.concatenate([mid, end], axis=0)
                before = pltpu.roll(full, 1, 0)
                after = pltpu.roll(full, RING - 1, 0)
                for s, v in enumerate((before, full, after)):
                    sb[t, p, :, pl.ds(384 * e + 128 * s, 128)] = v[0:TW].astype(bf16)
        return 0

    lax.fori_loop(0, 9, norm2, 0)

    def conv2(step, _):
        t, p0 = step // 2, 4 * lax.rem(step, 2)
        acc = jnp.dot(sb[t, pl.ds(p0, 4)].reshape(4 * TW, 768), w2[0], preferred_element_type=f32)
        acc += jnp.dot(sb[t, pl.ds(p0 + 1, 4)].reshape(4 * TW, 768), w2[1], preferred_element_type=f32)
        y = (acc + bias2).reshape(4, TW, 256)
        for pp in range(4):
            for e in range(2):
                r = 2 * (p0 + pp) + e
                v = y[pp, :, 128 * e : 128 * e + 128] + xe[t, 2 + r].astype(f32)
                m = jnp.where(r < jnp.where(t == 0, rows[0], rows[1]), 1.0, 0.0).astype(f32)
                out[t, r] = (v * m).astype(bf16)
        return 0

    lax.fori_loop(0, 4, conv2, 0)

    got = p1.at[pl.ds(0, 2 * (N - 1))]
    pltpu.make_async_copy(got, got, p1_send).wait()
    pltpu.make_async_copy(got, got, p2_send).wait()
    for which in range(2):
        got = st.at[which, pl.ds(0, N - 1)]
        pltpu.make_async_copy(got, got, st_ssem.at[which]).wait()

    @pl.when(lax.rem(me, 4) == 0)
    def _():
        got = cst.at[pl.ds(0, 7)]
        pltpu.make_async_copy(got, got, c1_send).wait()
        got = c2s.at[pl.ds(0, N - 1)]
        pltpu.make_async_copy(got, got, c2_send).wait()

    @pl.when(lax.rem(me, 4) != 0)
    def _():
        pltpu.make_async_copy(cst, cst, c1_send).wait()


def shards(x, nb, vr, ti, gain1, shift1, kernel1, off1, gain2, shift2, kernel2, off2):
    vmem = pl.BlockSpec(memory_space=pltpu.VMEM)
    hbm = pl.BlockSpec(memory_space=pltpu.HBM)
    dma = pltpu.SemaphoreType.DMA
    row = lambda v: v.reshape(1, C)
    pin = lambda v: pltpu.with_memory_space_constraint(v, pltpu.HBM)
    return pl.pallas_call(
        kernel,
        out_shape=jax.ShapeDtypeStruct(x.shape, x.dtype),
        in_specs=[hbm] * 12,
        out_specs=vmem,
        scratch_shapes=[
            pltpu.SMEM((4, TILES), jnp.int32),
            pltpu.SMEM((TILES,), jnp.int32),
            pltpu.SMEM((TILES,), jnp.int32),
        ]
        + [pltpu.VMEM((1, C), f32)] * 6
        + [
            pltpu.VMEM((2, TH + 4, TW, C), bf16),
            pltpu.VMEM((TILES, 16, C), bf16),
            pltpu.VMEM((N, 2, 16, C), bf16),
            pltpu.VMEM((8, 2, 8, C), bf16),
            pltpu.VMEM((TILES, 8, C), bf16),
            pltpu.VMEM((N, 2, 2, 8, C), bf16),
            pltpu.VMEM((8, 2, 2, 8, C), bf16),
            pltpu.VMEM((2, 20 * 16, C), f32),
            pltpu.VMEM((2, 10, RING, 768), bf16),
            pltpu.VMEM((2, 9, TW, 768), bf16),
            pltpu.VMEM((2, 18, RING, C), bf16),
            pltpu.VMEM((2, 768, 256), bf16),
            pltpu.VMEM((2, 768, 256), bf16),
            pltpu.VMEM((2, TH * 16, C), f32),
            pltpu.VMEM((2, 1, C), f32),
            pltpu.VMEM((2, N, 1, C), f32),
            pltpu.VMEM((2, N, C), f32),
            pltpu.VMEM((N, C), f32),
            dma,
            dma((9,)),
            dma((12,)),
            dma,
            dma,
            dma,
            dma,
            dma,
            dma,
            dma,
            dma,
            dma((2,)),
            dma((2,)),
        ],
        compiler_params=pltpu.CompilerParams(
            collective_id=0, has_side_effects=True, vmem_limit_bytes=40 * 1024 * 1024
        ),
    )(
        *(
            pin(v)
            for v in (
                x, nb.T, vr, ti, row(gain1), row(shift1), kernel1.reshape(3, 3 * C, C), row(off1),
                row(gain2), row(shift2), kernel2.reshape(3, 3 * C, C), row(off2),
            )
        )
    )


def solution(mesh):
    in_specs = (P(("rep", "tile"), None, None, None), P("rep", None), P("rep"), P("rep")) + (P(),) * 8
    out_specs = P(("rep", "tile"), None, None, None)
    return jax.shard_map(shards, mesh=mesh, in_specs=in_specs, out_specs=out_specs, check_vma=False)
```
